32 devices in a mesh: groups: 2 (over y), gx: 16 (over z, x, core).
Axes of the slice: x: 2, y: 2, z: 4, core: 2. Of those that a mesh axis runs over, the one named last changes fastest.
Arguments:
- features: float32 [48, 64, 96, 128], P(None, ('groups', 'gx')), parts along dimension 1, may hold values from -6 to 6
- fine_weights: bfloat16 [1536, 8, 48, 48], P('gx'), may hold values from -1.796875 to 1.796875
- middle_weights: bfloat16 [384, 4, 48, 48], P('gx'), may hold values from -3 to 3
- lift_fine: float32 [48, 48], replicated, may hold values from -0.875 to 0.875
- lift_middle: float32 [48, 48], replicated, may hold values from -0.875 to 0.875
- project_out: float32 [48, 48], replicated, may hold values from -0.875 to 0.875
Outputs:
- result: float32 [48, 64, 96, 128], P(None, ('groups', 'gx')), parts along dimension 1
The draws below stay inside these ranges and needn't reach their ends.
There are 2 independent parts, one for each index of `groups`. The reference program is written for one: setup_inputs(seed, part) draws one part's arguments, and reference() takes and returns one part's arrays. A program takes and returns all parts, laid end to end along the dimension named above; an argument that names none is the same for every part. Nothing has to cross between parts.
All inputs are finite; a program needn't handle non-finite values.
Results may differ from the reference program's by a relative error of at most 0.0018.
Values sent between devices are 32-bit elements; how exact they have to be, the bound alone decides.
No kernel may reach another device: no remote copies, remote signals or barrier semaphores. Data moves between devices by JAX's collectives and lax.ppermute only.
A program may use at most 128 MiB of HBM per device.

```python
import jax
import jax.numpy as jnp
from jax import lax

C = 48
NY = 96
NZ = 128
KY = 48
KZ = 32
NX = 32
KX = 8
KX2 = 4
MODES = 1536
MODES2 = 384


def levels(own_key, dims, split, smallest, top_value):
    loudness = 1.0
    for dim, parts in split:
        steps = jax.random.uniform(jax.random.fold_in(jax.random.fold_in(own_key, 6), dim), (parts,), jnp.float32, smallest / len(split), top_value / len(split))
        loudness = loudness * jnp.repeat(jnp.exp(steps), dims[dim] // parts).reshape((-1,) + (1,) * (len(dims) - 1 - dim))
    return loudness


def normal_values(own_key, dims, scale, limit, split=(), kind=jnp.bfloat16):
    drawn = scale * jax.random.normal(own_key, dims, jnp.float32)
    if split:
        drawn = drawn * levels(own_key, dims, split, -0.22, 0.18)
    return jnp.clip(drawn, -limit, limit).astype(kind)


def setup_inputs(seed: int = 0, part: int = 0) -> dict:
    streams_of = jax.random.split(jax.random.key(seed), 7)
    part_keys = jax.random.split(jax.random.fold_in(streams_of[6], part), 7)
    features = normal_values(part_keys[0], (C, NX, NY, NZ), 1.0, 6.0, ((1, 16),), jnp.float32)
    fine_weights = normal_values(streams_of[1], (MODES, KX, C, C), 0.3, 1.796875, ((0, 16),))
    middle_weights = normal_values(streams_of[2], (MODES2, KX2, C, C), 0.5, 3.0, ((0, 16),))
    lift_fine = normal_values(streams_of[3], (C, C), C ** -0.5, 0.875, (), jnp.float32)
    lift_middle = normal_values(streams_of[4], (C, C), C ** -0.5, 0.875, (), jnp.float32)
    project_out = normal_values(streams_of[5], (C, C), C ** -0.5, 0.875, (), jnp.float32)
    return dict(features=features, fine_weights=fine_weights, middle_weights=middle_weights, lift_fine=lift_fine, lift_middle=lift_middle, project_out=project_out)


HIGHEST = lax.Precision.HIGHEST

def cosine_table(modes_kept, length, offset, columns):
    orders = jnp.arange(modes_kept, dtype=jnp.int32)[:, None]
    points = offset + jnp.arange(columns, dtype=jnp.int32)[None, :]
    phase = orders * (2 * points + 1) % (4 * length)
    angle = jnp.pi / (2 * length) * phase.astype(jnp.float32)
    scales = jnp.where(orders == 0, jnp.sqrt(jnp.float32(1.0 / length)), jnp.sqrt(jnp.float32(2.0 / length)))
    return scales.astype(jnp.float32) * jnp.cos(angle)

def forward_yz(values, modes_y, modes_z):
    channels, local_x, cells_y, cells_z = values.shape
    table_z = cosine_table(modes_z, cells_z, 0, cells_z)
    table_y = cosine_table(modes_y, cells_y, 0, cells_y)
    along_z = jnp.einsum('cxyz,jz->cxyj', values, table_z, precision=HIGHEST)
    both = jnp.einsum('cxyj,iy->ijxc', along_z, table_y, precision=HIGHEST)
    return both.reshape(modes_y * modes_z, local_x, channels)

def inverse_yz(coeffs, modes_y, modes_z, cells_y, cells_z):
    total, local_x, channels = coeffs.shape
    shaped = coeffs.reshape(modes_y, modes_z, local_x, channels)
    table_z = cosine_table(modes_z, cells_z, 0, cells_z)
    table_y = cosine_table(modes_y, cells_y, 0, cells_y)
    along_y = jnp.einsum('ijxc,iy->jxcy', shaped, table_y, precision=HIGHEST)
    return jnp.einsum('jxcy,jz->cxyz', along_y, table_z, precision=HIGHEST)

def spectral(values, weights, modes_x, modes_y, modes_z):
    channels, cells_x, cells_y, cells_z = values.shape
    coeffs = forward_yz(values, modes_y, modes_z)
    table_x = cosine_table(modes_x, cells_x, 0, cells_x)
    modal = jnp.einsum('mxc,kx->mkc', coeffs, table_x, precision=HIGHEST)
    modal_b = modal.astype(jnp.bfloat16)
    mixed = jnp.einsum('mkc,mkco->mko', modal_b.astype(jnp.float32), weights.astype(jnp.float32), precision=HIGHEST)
    back = jnp.einsum('mkc,kx->mxc', mixed, table_x, precision=HIGHEST)
    return inverse_yz(back, modes_y, modes_z, cells_y, cells_z)

def pointwise(values, matrix):
    return jnp.einsum('cxyz,co->oxyz', values, matrix, precision=HIGHEST)

def coarsen(values):
    channels, cells_x, cells_y, cells_z = values.shape
    shaped = values.reshape(channels, cells_x // 2, 2, cells_y // 2, 2, cells_z // 2, 2)
    return lax.optimization_barrier(jnp.mean(shaped, axis=(2, 4, 6)))

def refine(values):
    return jnp.repeat(jnp.repeat(jnp.repeat(values, 2, axis=1), 2, axis=2), 2, axis=3)

def reference(features, fine_weights, middle_weights, lift_fine, lift_middle, project_out):
    level_one = jax.nn.gelu(spectral(features, fine_weights, KX, KY, KZ) + pointwise(features, lift_fine), approximate=False)
    pooled = coarsen(level_one)
    level_two = jax.nn.gelu(spectral(pooled, middle_weights, KX2, KY // 2, KZ // 2) + pointwise(pooled, lift_middle), approximate=False)
    return features + pointwise(level_one + refine(level_two), project_out)
```

```python
import jax
import jax.numpy as jnp
import numpy as np
from jax import lax
from jax.experimental import pallas as pl
from jax.experimental.pallas import tpu as pltpu
from jax.sharding import PartitionSpec as P

KY = 48
KZ = 32
LANES = 128
PAD = 16
GROUP = 16
HIGHEST = lax.Precision.HIGHEST
BF = jnp.bfloat16
F32 = jnp.float32
MIB = 1 << 20


def cosine(modes_kept, length):
    orders = np.arange(modes_kept)[:, None]
    points = np.arange(length)[None, :]
    phase = orders * (2 * points + 1) % (4 * length)
    scales = np.where(orders == 0, np.sqrt(1.0 / length), np.sqrt(2.0 / length))
    return scales * np.cos(np.pi / (2 * length) * phase)


def halves(table):
    table = np.asarray(table, np.float32)
    high = table.astype(BF)
    low = (table - high.astype(np.float32)).astype(BF)
    return high, low


def split(values):
    high = values.astype(BF)
    return high, (values - high.astype(F32)).astype(BF)


def dot(a, b):
    return jnp.dot(a, b, preferred_element_type=F32)


def gelu(t):
    return 0.5 * t * (1.0 + lax.erf(t * np.float32(np.sqrt(0.5))))


def vmem_call(body, outs, args, scratch, limit, hbm_out=False):
    in_vmem = pl.BlockSpec(memory_space=pltpu.VMEM)
    out_specs = tuple(
        pl.BlockSpec(memory_space=pl.ANY if hbm_out else pltpu.VMEM) for _ in outs
    )
    shapes = tuple(jax.ShapeDtypeStruct(s, F32) for s in outs)
    single = len(outs) == 1
    return pl.pallas_call(
        body,
        out_shape=shapes[0] if single else shapes,
        in_specs=[in_vmem] * len(args),
        out_specs=out_specs[0] if single else out_specs,
        scratch_shapes=scratch,
        compiler_params=pltpu.CompilerParams(vmem_limit_bytes=limit * MIB),
        name=body.__name__,
    )(*args)


def interleave_matrix(matrix, factor, transposed_rows):
    channels = matrix.shape[0]
    rows = channels * 8 * factor
    cols = channels * 8
    spread_rows = (
        lax.broadcasted_iota(jnp.int32, (channels, rows), 1) // (8 * factor)
        == lax.broadcasted_iota(jnp.int32, (channels, rows), 0)
    )
    spread_cols = (
        lax.broadcasted_iota(jnp.int32, (channels, cols), 1) // 8
        == lax.broadcasted_iota(jnp.int32, (channels, cols), 0)
    ).astype(F32).astype(BF)
    spread_rows = spread_rows.astype(F32).astype(BF)
    keep = (
        lax.broadcasted_iota(jnp.int32, (rows, cols), 0) % (8 * factor) // factor
        == lax.broadcasted_iota(jnp.int32, (rows, cols), 1) % 8
    )
    parts = []
    for part in split(matrix):
        tall = lax.dot_general(part, spread_cols, (((0,), (0,)), ((), ())), preferred_element_type=F32)
        wide = lax.dot_general(
            spread_rows, tall.astype(BF), (((0,), (0,)), ((), ())), preferred_element_type=F32
        )
        parts.append(jnp.where(keep, wide, 0.0).astype(BF))
    return parts


def forward_fine(v_ref, wz_ref, ty_ref, out_ref, z_ref):
    channels, local_x, cells_y, cells_z = v_ref.shape
    half = channels // 2
    chunk = 6
    for first in range(0, half, chunk):
        rows = [
            jnp.concatenate(
                [v_ref[c, x] for c in (cp, cp + half) for x in range(local_x)], axis=1
            )
            for cp in range(first, first + chunk)
        ]
        high, low = split(jnp.concatenate(rows, axis=0))
        wide = dot(high, wz_ref[...])
        total = wide[:, :LANES] + wide[:, LANES:] + dot(low, wz_ref[:, :LANES])
        for n in range(chunk):
            z_ref[first + n] = total[n * cells_y : (n + 1) * cells_y]
    modes_y = ty_ref.shape[0] // 2
    for cp in range(0, half, 2):
        high, low = split(jnp.concatenate([z_ref[cp], z_ref[cp + 1]], axis=1))
        both = dot(ty_ref[...], jnp.concatenate([high, low], axis=0))
        both = both[:modes_y] + both[modes_y:]
        for n in range(2):
            out_ref[pl.ds(cp + n, modes_y, stride=half), :] = both[:, n * LANES : (n + 1) * LANES]


def fine_coefficients(features):
    channels, local_x, cells_y, cells_z = features.shape
    high, low = halves(cosine(KZ, cells_z).T)
    eye = np.eye(2 * local_x, dtype=np.float32)
    wz = np.concatenate(
        [np.kron(eye, part.astype(np.float32)) for part in (high, low)], axis=1
    ).astype(BF)
    high, low = halves(cosine(KY, cells_y))
    ty = np.block([[high, high], [low, np.zeros_like(low)]]).astype(BF)
    return vmem_call(
        forward_fine,
        [(KY * channels // 2, LANES)],
        (features, jnp.asarray(wz), jnp.asarray(ty)),
        [pltpu.VMEM((channels // 2, cells_y, LANES), F32)],
        24,
    )


def mix_fine(r_ref, w_ref, tv_ref, out_ref, modal_ref, mixed_ref, spread_ref):
    members, rows, _ = r_ref.shape
    modes_x, channels, _, owned = w_ref.shape
    half = channels // 2
    per = owned // KZ
    quarter = lax.broadcasted_iota(jnp.int32, (half, LANES), 1) // KZ
    for first in range(0, modes_x, 4):
        acc = [None] * 4
        for a in range(members):
            block = r_ref[a]
            for n in range(4):
                term = block * tv_ref[(first + n) * members + a][None, :]
                acc[n] = term if a == 0 else acc[n] + term
        for n in range(4):
            both = acc[n] + pltpu.roll(acc[n], LANES - KZ, 1)
            for c2 in range(2):
                placed = None
                for i in range(per):
                    piece = both[i * half : (i + 1) * half]
                    shift = (KZ * i - 2 * KZ * c2) % LANES
                    piece = pltpu.roll(piece, shift, 1) if shift else piece
                    placed = piece if placed is None else jnp.where(quarter == i, piece, placed)
                modal_ref[first + n, c2 * half : (c2 + 1) * half, :] = placed.astype(BF).astype(F32)

    def one_mode(k, carry):
        total = None
        for c in range(channels):
            term = modal_ref[k, c : c + 1, :owned] * w_ref[k, c].astype(F32)
            total = term if total is None else total + term
        mixed_ref[k, :, :owned] = total
        return carry

    lax.fori_loop(0, modes_x, one_mode, 0)
    for k in range(modes_x):
        for i in range(per):
            placed = None
            for q in range(4):
                c2 = q // 2
                piece = mixed_ref[k, c2 * half : (c2 + 1) * half, :]
                shift = (KZ * q - KZ * i) % LANES
                piece = pltpu.roll(piece, shift, 1) if shift else piece
                placed = piece if placed is None else jnp.where(quarter == q, piece, placed)
            spread_ref[k, i * half : (i + 1) * half, :] = placed
    for a in range(members):
        total = None
        for k in range(modes_x):
            term = spread_ref[k] * tv_ref[k * members + a][None, :]
            total = term if total is None else total + term
        out_ref[a] = total


def fine_mixed(received, weights, local_x):
    members, rows, _ = received.shape
    owned, modes_x, channels, _ = weights.shape
    table = cosine(modes_x, members * local_x).reshape(modes_x * members, local_x)
    lanes = np.tile(np.repeat(table, KZ, axis=1), (1, 2)).astype(np.float32)
    return vmem_call(
        mix_fine,
        [received.shape],
        (received, jnp.transpose(weights, (1, 2, 3, 0)), jnp.asarray(lanes)),
        [
            pltpu.VMEM((modes_x, channels, LANES), F32),
            pltpu.VMEM((modes_x, channels, LANES), F32),
            pltpu.VMEM((modes_x, rows, LANES), F32),
        ],
        16,
    )


def lift_blocks(source, parts, cells_y, store):
    channels = source.shape[0]
    for y in range(0, cells_y, 16):
        block = jnp.concatenate(
            [source[:, y + s : y + s + 8, :].reshape(channels * 8, LANES) for s in (0, 8)], axis=1
        )
        high, low = split(block)
        done = dot(parts[0], high) + dot(parts[1], high) + dot(parts[0], low)
        rows = done.shape[0] // channels
        for n in range(2):
            store(y + 8 * n, done[:, n * LANES : (n + 1) * LANES].reshape(channels, rows, LANES))


def lift_fine_kernel(v_ref, a_ref, out_ref):
    parts = interleave_matrix(a_ref[...], 1, False)
    for x in range(v_ref.shape[1]):
        def store(y, value, x=x):
            out_ref[:, x, y : y + 8, :] = value
        lift_blocks(v_ref.at[:, x], parts, v_ref.shape[2], store)


def project_kernel(v_ref, a_ref, base_ref, out_ref):
    parts = interleave_matrix(a_ref[...], 1, False)
    for x in range(v_ref.shape[1]):
        def store(y, value, x=x):
            out_ref[:, x, y : y + 8, :] = value + base_ref[:, x, y : y + 8, :]
        lift_blocks(v_ref.at[:, x], parts, v_ref.shape[2], store)


def lift_coarse_kernel(v_ref, a_ref, pz_ref, out_ref, p_ref):
    parts = interleave_matrix(a_ref[...], 1, False)
    channels, cells_y, _ = v_ref.shape

    def store(y, value):
        p_ref[:, y : y + 8, :] = value

    lift_blocks(v_ref, parts, cells_y, store)
    rows = jnp.concatenate(
        [jnp.concatenate([p_ref[c], p_ref[c + 1]], axis=1) for c in range(0, channels, 2)], axis=0
    )
    high, low = split(rows)
    done = dot(high, pz_ref[...]) + dot(low, pz_ref[...])
    for cg in range(channels // GROUP):
        for t in range(GROUP // 2):
            n = cg * (GROUP // 2) + t
            out_ref[cg * cells_y : (cg + 1) * cells_y, t * LANES : (t + 1) * LANES] = done[
                n * cells_y : (n + 1) * cells_y
            ]


def inverse_fine(r_ref, lift_ref, ty_ref, bz_ref, yc_ref, ec_ref, level_ref, pool_ref, out_ref,
                 g_ref, q_ref, w_ref, d_ref, place):
    channels, local_x, cells_y, cells_z = lift_ref.shape
    half = channels // 2
    modes_y = r_ref.shape[0] // half
    half_ky = modes_y // 2
    coarse_y = cells_y // 2
    for cp in range(0, half, 2):
        block = jnp.concatenate(
            [r_ref[pl.ds(cp + n, modes_y, stride=half), :] for n in range(2)], axis=1
        )
        high, low = split(block)
        both = dot(ty_ref[...], jnp.concatenate([high, low, high], axis=0)).astype(BF)
        for n in range(2):
            part = both[:, n * LANES : (n + 1) * LANES]
            g_ref[(cp + n) * cells_y : (cp + n + 1) * cells_y, :] = jnp.concatenate(
                [part, part], axis=1
            )
    lane = lax.broadcasted_iota(jnp.int32, (cells_z, 2 * LANES), 1) % GROUP
    for c in range(GROUP):
        for part in range(2):
            w_ref[part, c * cells_z : (c + 1) * cells_z, :] = jnp.where(
                lane == c, ec_ref[part].astype(F32), 0.0
            ).astype(BF)
    chunk = 4
    for first in range(0, half, chunk):
        wide = dot(g_ref[first * cells_y : (first + chunk) * cells_y, :], bz_ref[...])
        for n in range(chunk):
            cp = first + n
            tall = []
            for c2 in range(2):
                column = []
                for x in range(local_x):
                    q = c2 * local_x + x
                    piece = wide[n * cells_y : (n + 1) * cells_y, q * LANES : (q + 1) * LANES]
                    piece = gelu(piece + lift_ref[cp + c2 * half, x])
                    level_ref[cp + c2 * half, x] = piece
                    column.append(piece.astype(BF))
                tall.append(jnp.concatenate(column, axis=0))
            down = dot(yc_ref[...], jnp.concatenate(tall, axis=1))
            for c2 in range(2):
                c = cp + c2 * half
                cg, inner = c // GROUP, c % GROUP
                part = down[:, c2 * LANES : (c2 + 1) * LANES]
                q_ref[cg * half_ky : (cg + 1) * half_ky, inner * LANES : (inner + 1) * LANES] = (
                    part[:half_ky] + part[half_ky : 2 * half_ky]
                )
                pool_ref[c] = part[2 * half_ky :]
    high, low = split(q_ref[...])
    d_ref[...] = dot(high, w_ref[0]) + dot(low, w_ref[0]) + dot(high, w_ref[1])
    out_ref[...] = jnp.zeros_like(out_ref)
    for (cg, jh, i), row in place.items():
        source = cg * half_ky + i
        out_ref[row : row + 1, :] = d_ref[source : source + 1, jh * LANES : (jh + 1) * LANES]


def fine_level(received, lifted, place, place_rows):
    channels, local_x, cells_y, cells_z = lifted.shape
    half_ky, half_kz = KY // 2, KZ // 2
    coarse_y, coarse_z = cells_y // 2, cells_z // 2
    high, low = halves(cosine(KY, cells_y).T)
    ty = np.concatenate([high, high, low], axis=1)
    eye = np.eye(2 * local_x, dtype=np.float32)
    bz = np.concatenate(
        [np.kron(eye, part.astype(np.float32)) for part in halves(cosine(KZ, cells_z))], axis=0
    ).astype(BF)
    pool_y = np.kron(np.eye(coarse_y), np.ones((1, 2))) / (2.0 * local_x)
    pool_z = np.kron(np.eye(coarse_z), np.ones((1, 2))) / 2.0
    high, low = halves(cosine(half_ky, coarse_y) @ pool_y)
    yc = np.concatenate([high, low, pool_y.astype(BF)], axis=0)
    yc = np.concatenate([yc] * local_x, axis=1)
    ec = np.repeat((cosine(half_kz, coarse_z) @ pool_z).T, GROUP, axis=1)
    ec = np.stack(halves(ec))
    groups = channels // GROUP

    def inverse_fine_kernel(*refs):
        inverse_fine(*refs, place)

    return vmem_call(
        inverse_fine_kernel,
        [lifted.shape, (channels, coarse_y, cells_z), (place_rows, LANES)],
        (received, lifted, jnp.asarray(ty), jnp.asarray(bz), jnp.asarray(yc), jnp.asarray(ec)),
        [
            pltpu.VMEM((channels // 2 * cells_y, 2 * LANES), BF),
            pltpu.VMEM((groups * half_ky, GROUP * cells_z), F32),
            pltpu.VMEM((2, GROUP * cells_z, 2 * LANES), BF),
            pltpu.VMEM((groups * half_ky, 2 * LANES), F32),
        ],
        28,
    )


def mix_coarse(r_ref, w_ref, out_ref, table, rows):
    members, pad, _ = r_ref.shape
    owned, modes_x, channels, _ = w_ref.shape
    groups = channels // GROUP
    inner = LANES // GROUP
    units = owned // inner
    lane = lax.broadcasted_iota(jnp.int32, (rows, LANES), 1)
    row = lax.broadcasted_iota(jnp.int32, (rows, channels), 0)
    modal = []
    for k in range(modes_x):
        total = None
        for a in range(members):
            term = r_ref[a] * float(table[k, a])
            total = term if total is None else total + term
        modal.append(total)
    fill = jnp.zeros((rows - modes_x * units, LANES), F32)
    packed = [
        jnp.concatenate(
            [modal[k][cg * units : (cg + 1) * units] for k in range(modes_x)] + [fill], axis=0
        )
        for cg in range(groups)
    ]
    mixed = []
    for j in range(inner):
        placed = None
        for cg in range(groups):
            shift = (GROUP * cg - GROUP * j) % LANES
            piece = pltpu.roll(packed[cg], shift, 1) if shift else packed[cg]
            placed = piece if placed is None else jnp.where(lane // GROUP == cg, piece, placed)
        left = placed[:, :channels].astype(BF)
        total = jnp.zeros((rows, channels), F32)
        for k in range(modes_x):
            for u in range(units):
                full = dot(left, w_ref[u * inner + j, k])
                total = jnp.where(row == k * units + u, full, total)
        mixed.append(jnp.concatenate([total, jnp.zeros((rows, LANES - channels), F32)], axis=1))
    spread = []
    for cg in range(groups):
        placed = None
        for j in range(inner):
            shift = (GROUP * j - GROUP * cg) % LANES
            piece = pltpu.roll(mixed[j], shift, 1) if shift else mixed[j]
            placed = piece if placed is None else jnp.where(lane // GROUP == j, piece, placed)
        spread.append(placed)
    final = []
    for k in range(modes_x):
        final.append(
            jnp.concatenate(
                [spread[cg][k * units : (k + 1) * units] for cg in range(groups)]
                + [jnp.zeros((pad - groups * units, LANES), F32)],
                axis=0,
            )
        )
    for a in range(members):
        total = None
        for k in range(modes_x):
            term = final[k] * float(table[k, a])
            total = term if total is None else total + term
        out_ref[a] = total


def coarse_mixed(received, weights, coarse_x):
    owned, modes_x, channels, _ = weights.shape
    table = cosine(modes_x, coarse_x)
    units = owned * GROUP // LANES
    rows = -(-modes_x * units // 16) * 16

    def mix_coarse_kernel(*refs):
        mix_coarse(*refs, table, rows)

    return vmem_call(mix_coarse_kernel, [received.shape], (received, weights), [], 16)


def finish(r_ref, lift_ref, base_ref, a_ref, yi_ref, ei_ref, up_ref, out_ref, b_ref, l_ref, res_ref, sems):
    channels, local_x, cells_y, cells_z = base_ref.shape
    coarse_y = cells_y // 2
    groups = channels // GROUP
    coarse_z = cells_z // 2
    lane = lax.broadcasted_iota(jnp.int32, (2 * LANES, LANES), 1) // coarse_z
    row = lax.broadcasted_iota(jnp.int32, (2 * LANES, LANES), 0) % GROUP
    for t in range(GROUP // 2):
        for part in range(2):
            b_ref[part, :, t * LANES : (t + 1) * LANES] = jnp.where(
                row == 2 * t + lane, ei_ref[part].astype(F32), 0.0
            ).astype(BF)
    high, low = split(r_ref[...])
    grid = dot(yi_ref[0], high) + dot(yi_ref[0], low) + dot(yi_ref[1], high)
    left = jnp.concatenate(
        [
            jnp.concatenate(
                [grid[(2 * cg + jh) * coarse_y : (2 * cg + jh + 1) * coarse_y] for jh in range(2)],
                axis=1,
            )
            for cg in range(groups)
        ],
        axis=0,
    )
    high, low = split(left)
    level = dot(high, b_ref[0]) + dot(low, b_ref[0]) + dot(high, b_ref[1])
    level = gelu(level + lift_ref[...])
    for cg in range(groups):
        tall = jnp.concatenate(
            [
                level[cg * coarse_y : (cg + 1) * coarse_y, t * LANES : (t + 1) * LANES]
                for t in range(GROUP // 2)
            ],
            axis=0,
        )
        high, low = split(tall)
        wide = dot(jnp.concatenate([high, low], axis=1), up_ref[...])
        for t in range(GROUP // 2):
            for c2 in range(2):
                l_ref[cg * GROUP + 2 * t + c2] = wide[
                    t * coarse_y : (t + 1) * coarse_y, c2 * LANES : (c2 + 1) * LANES
                ]
    parts = interleave_matrix(a_ref[...], 2, False)
    copies = []

    def store(y, value):
        for x in range(local_x):
            res_ref[:, x, 2 * y : 2 * y + 16, :] = value + base_ref[:, x, 2 * y : 2 * y + 16, :]
        if y % 16 == 8:
            span = pl.ds(2 * y - 16, 32)
            copy = pltpu.make_async_copy(
                res_ref.at[:, :, span, :], out_ref.at[:, :, span, :], sems.at[y // 16]
            )
            copy.start()
            copies.append(copy)

    lift_blocks(l_ref, parts, coarse_y, store)
    for copy in copies:
        copy.wait()


def final_result(received, lifted, base, matrix, place, place_rows):
    channels, local_x, cells_y, cells_z = base.shape
    half_ky, half_kz = KY // 2, KZ // 2
    coarse_y, coarse_z = cells_y // 2, cells_z // 2
    groups = channels // GROUP
    table_y = cosine(half_ky, coarse_y)
    left = np.zeros((groups, 2, coarse_y, place_rows))
    for (cg, jh, i), row in place.items():
        left[cg, jh, :, row] = table_y[i]
    yi = np.stack(halves(left.reshape(groups * 2 * coarse_y, place_rows)))
    inverse_z = np.repeat(cosine(half_kz, coarse_z), GROUP, axis=0)
    ei = np.stack(halves(np.concatenate([inverse_z] * (LANES // coarse_z), axis=1)))
    up = np.kron(np.eye(2), np.kron(np.eye(coarse_z), np.ones((1, 2))))
    up = np.concatenate([up, up], axis=0).astype(BF)
    args = (received, lifted, base, matrix, jnp.asarray(yi), jnp.asarray(ei), jnp.asarray(up))
    return vmem_call(
        finish,
        [base.shape],
        args,
        [
            pltpu.VMEM((2, 2 * LANES, GROUP // 2 * LANES), BF),
            pltpu.VMEM((channels, coarse_y, cells_z), F32),
            pltpu.VMEM(base.shape, F32),
            pltpu.SemaphoreType.DMA((coarse_y // 16,)),
        ],
        32,
        hbm_out=True,
    )


def swap(blocks):
    return lax.all_to_all(blocks, "gx", split_axis=0, concat_axis=0, tiled=True)


def plain_mix(coeffs, weights, cells_x):
    group_size = lax.axis_size("gx")
    table_x = jnp.asarray(cosine(weights.shape[1], cells_x), F32)
    pencils = lax.all_to_all(coeffs, "gx", split_axis=0, concat_axis=1, tiled=True)
    modal = jnp.einsum("mxc,kx->mkc", pencils, table_x, precision=HIGHEST)
    mixed = jnp.einsum(
        "mkc,mkco->mko", modal.astype(BF), weights, preferred_element_type=F32
    )
    back = jnp.einsum("mkc,kx->mxc", mixed, table_x, precision=HIGHEST)
    return lax.all_to_all(back, "gx", split_axis=1, concat_axis=0, tiled=True)


def on_device(features, fine_weights, middle_weights, lift_fine, lift_middle, project_out):
    channels, local_x, cells_y, cells_z = features.shape
    group_size = lax.axis_size("gx")
    cells_x = local_x * group_size
    half = channels // 2
    half_ky, half_kz = KY // 2, KZ // 2
    groups = channels // GROUP
    inner = LANES // GROUP

    coeffs = fine_coefficients(features)
    owned = fine_weights.shape[0]
    if owned % KZ == 0 and owned <= LANES:
        received = swap(coeffs.reshape(group_size, -1, LANES))
        mixed = fine_mixed(received, fine_weights, local_x)
        slabs = swap(mixed).reshape(coeffs.shape)
    else:
        modes = coeffs.reshape(KY, half, 2, local_x, KZ).transpose(0, 4, 3, 2, 1)
        slabs = plain_mix(modes.reshape(KY * KZ, local_x, channels), fine_weights, cells_x)
        slabs = slabs.reshape(KY, KZ, local_x, 2, half).transpose(0, 4, 3, 2, 1)
        slabs = slabs.reshape(coeffs.shape)
    lifted = vmem_call(lift_fine_kernel, [features.shape], (features, lift_fine), [], 24)

    owned = middle_weights.shape[0]
    direct = owned % inner == 0 and groups * (owned // inner) <= PAD
    place = {}
    for cg in range(groups):
        for i in range(half_ky):
            for jh in range(2):
                if direct:
                    member, unit = divmod(2 * i + jh, owned // inner)
                    place[cg, jh, i] = member * PAD + cg * (owned // inner) + unit
                else:
                    place[cg, jh, i] = (jh * groups + cg) * half_ky + i
    place_rows = group_size * PAD if direct else 2 * groups * half_ky
    level_one, pool_y, coarse = fine_level(slabs, lifted, place, place_rows)
    base = vmem_call(project_kernel, [features.shape], (level_one, project_out, features), [], 28)
    pool_z = np.kron(np.eye(cells_z // 2), np.ones((1, 2))).T / 2.0
    pool_z = jnp.asarray(np.kron(np.eye(2), pool_z).astype(BF))
    coarse_lift = vmem_call(
        lift_coarse_kernel,
        [(groups * cells_y // 2, GROUP // 2 * LANES)],
        (pool_y, lift_middle, pool_z),
        [pltpu.VMEM(pool_y.shape, F32)],
        16,
    )
    coarse_x = cells_x // 2
    if direct:
        received = swap(coarse.reshape(group_size, PAD, LANES))
        mixed = coarse_mixed(received, middle_weights, coarse_x)
        slabs = swap(mixed).reshape(coarse.shape)
    else:
        modes = coarse.reshape(2, groups, half_ky, inner, GROUP).transpose(2, 0, 3, 1, 4)
        slabs = plain_mix(
            modes.reshape(half_ky * half_kz, 1, channels), middle_weights, coarse_x
        )
        slabs = slabs.reshape(half_ky, 2, inner, groups, GROUP).transpose(1, 3, 0, 2, 4)
        slabs = slabs.reshape(coarse.shape)
    return final_result(slabs, coarse_lift, base, project_out, place, place_rows)


def solution(mesh):
    in_specs = (
        P(None, ("groups", "gx"), None, None),
        P("gx", None, None, None),
        P("gx", None, None, None),
        P(),
        P(),
        P(),
    )
    out_specs = P(None, ("groups", "gx"), None, None)
    return jax.shard_map(
        on_device, mesh=mesh, in_specs=in_specs, out_specs=out_specs, check_vma=False
    )
```

```python
import jax
import jax.numpy as jnp
import numpy as np
from jax import lax
from jax.experimental import pallas as pl
from jax.experimental.pallas import tpu as pltpu
from jax.sharding import PartitionSpec as P

KY = 48
KZ = 32
LANES = 128
PAD = 16
GROUP = 16
HIGHEST = lax.Precision.HIGHEST
BF = jnp.bfloat16
F32 = jnp.float32
MIB = 1 << 20
LIFT_FLOPS = 1 << 32
FETCHES = 3


def cosine(modes_kept, length):
    orders = np.arange(modes_kept)[:, None]
    points = np.arange(length)[None, :]
    phase = orders * (2 * points + 1) % (4 * length)
    scales = np.where(orders == 0, np.sqrt(1.0 / length), np.sqrt(2.0 / length))
    return scales * np.cos(np.pi / (2 * length) * phase)


def halves(table):
    table = np.asarray(table, np.float32)
    high = table.astype(BF)
    low = (table - high.astype(np.float32)).astype(BF)
    return high, low


def split(values):
    high = values.astype(BF)
    return high, (values - high.astype(F32)).astype(BF)


def dot(a, b):
    return jnp.dot(a, b, preferred_element_type=F32)


def gelu(t):
    return 0.5 * t * (1.0 + lax.erf(t * np.float32(np.sqrt(0.5))))


def paired(values):
    return values.reshape((2, values.shape[0] // 2) + values.shape[1:])


def vmem_call(body, outs, args, scratch, limit, flops=0, in_hbm=(), out_hbm=()):
    specs = [
        pl.BlockSpec(memory_space=pltpu.HBM if n in in_hbm else pltpu.VMEM) for n in range(len(args))
    ]
    out_specs = [
        pl.BlockSpec(memory_space=pltpu.HBM if n in out_hbm else pltpu.VMEM) for n in range(len(outs))
    ]
    shapes = [
        pltpu.HBM(shape, kind) if n in out_hbm else jax.ShapeDtypeStruct(shape, kind)
        for n, (shape, kind) in enumerate(outs)
    ]
    args = [
        pltpu.with_memory_space_constraint(a, pltpu.HBM) if n in in_hbm else a
        for n, a in enumerate(args)
    ]
    moved = sum(a.size * a.dtype.itemsize for a in args)
    result = pl.pallas_call(
        body,
        out_shape=shapes,
        in_specs=specs,
        out_specs=out_specs,
        scratch_shapes=scratch,
        compiler_params=pltpu.CompilerParams(vmem_limit_bytes=limit * MIB),
        cost_estimate=pl.CostEstimate(flops=flops, transcendentals=0, bytes_accessed=moved),
    )(*args)
    return result[0] if len(outs) == 1 else result


def interleave_matrix(matrix):
    channels = matrix.shape[0]
    size = channels * 8
    spread = (
        lax.broadcasted_iota(jnp.int32, (channels, size), 1) // 8
        == lax.broadcasted_iota(jnp.int32, (channels, size), 0)
    ).astype(F32).astype(BF)
    keep = (
        lax.broadcasted_iota(jnp.int32, (size, size), 0) % 8
        == lax.broadcasted_iota(jnp.int32, (size, size), 1) % 8
    )
    first = (((0,), (0,)), ((), ()))
    parts = []
    for part in split(matrix):
        tall = lax.dot_general(part, spread, first, preferred_element_type=F32).astype(BF)
        wide = lax.dot_general(spread, tall, first, preferred_element_type=F32)
        parts.append(jnp.where(keep, wide, 0.0).astype(BF))
    return parts


def forward_fine(hbm_ref, wz_hbm, ty_hbm, out_ref, z_ref, v_ref, wz_ref, ty_ref, sems):
    _, half, local_x, cells_y, _ = v_ref.shape
    steps = FETCHES
    chunk = half // steps
    tables = [
        pltpu.make_async_copy(wz_hbm, wz_ref, sems.at[steps]),
        pltpu.make_async_copy(ty_hbm, ty_ref, sems.at[steps + 1]),
    ]
    fetches = [
        pltpu.make_async_copy(hbm_ref.at[:, span], v_ref.at[:, span], sems.at[n])
        for n, span in enumerate(pl.ds(n * chunk, chunk) for n in range(steps))
    ]
    for copy in [tables[0], fetches[0], tables[1]] + fetches[1:]:
        copy.start()
    modes_y = ty_ref.shape[0] // 2

    def along_z(first):
        rows = [
            jnp.concatenate([v_ref[c2, cp, x] for c2 in range(2) for x in range(local_x)], axis=1)
            for cp in range(first, first + chunk)
        ]
        high, low = split(jnp.concatenate(rows, axis=0))
        wide = dot(high, wz_ref[...])
        total = wide[:, :LANES] + wide[:, LANES:] + dot(low, wz_ref[:, :LANES])
        for m in range(chunk):
            z_ref[first + m] = total[m * cells_y : (m + 1) * cells_y]

    def along_y(first):
        for cp in range(first, first + chunk, 2):
            high, low = split(jnp.concatenate([z_ref[cp], z_ref[cp + 1]], axis=1))
            both = dot(ty_ref[...], jnp.concatenate([high, low], axis=0))
            both = both[:modes_y] + both[modes_y:]
            for n in range(2):
                out_ref[pl.ds(cp + n, modes_y, stride=half), :] = both[
                    :, n * LANES : (n + 1) * LANES
                ]

    tables[0].wait()
    for n in range(steps):
        fetches[n].wait()
        if n == 1:
            tables[1].wait()
        if n:
            along_y((n - 1) * chunk)
        along_z(n * chunk)
    along_y((steps - 1) * chunk)


def fine_coefficients(features):
    channels, local_x, cells_y, cells_z = features.shape
    high, low = halves(cosine(KZ, cells_z).T)
    eye = np.eye(2 * local_x, dtype=np.float32)
    wz = np.concatenate(
        [np.kron(eye, part.astype(np.float32)) for part in (high, low)], axis=1
    ).astype(BF)
    high, low = halves(cosine(KY, cells_y))
    ty = np.block([[high, high], [low, np.zeros_like(low)]]).astype(BF)
    return vmem_call(
        forward_fine,
        [((KY * channels // 2, LANES), F32)],
        (paired(features), jnp.asarray(wz), jnp.asarray(ty)),
        [
            pltpu.VMEM((channels // 2, cells_y, LANES), F32),
            pltpu.VMEM(paired(features).shape, F32),
            pltpu.VMEM(wz.shape, BF),
            pltpu.VMEM(ty.shape, BF),
            pltpu.SemaphoreType.DMA((FETCHES + 2,)),
        ],
        16,
        in_hbm=(0, 1, 2),
    )


def mix_fine(r_ref, w_ref, tv_ref, out_ref, modal_ref, mixed_ref, spread_ref):
    members, _, _ = r_ref.shape
    modes_x, channels, _, owned = w_ref.shape
    half = channels // 2
    per = owned // KZ
    quarter = lax.broadcasted_iota(jnp.int32, (half, LANES), 1) // KZ
    for first in range(0, modes_x, 4):
        acc = [None] * 4
        for a in range(members):
            block = r_ref[a]
            for n in range(4):
                term = block * tv_ref[(first + n) * members + a][None, :]
                acc[n] = term if a == 0 else acc[n] + term
        for n in range(4):
            both = acc[n] + pltpu.roll(acc[n], LANES - KZ, 1)
            for c2 in range(2):
                placed = None
                for i in range(per):
                    piece = both[i * half : (i + 1) * half]
                    shift = (KZ * i - 2 * KZ * c2) % LANES
                    piece = pltpu.roll(piece, shift, 1) if shift else piece
                    placed = piece if placed is None else jnp.where(quarter == i, piece, placed)
                modal_ref[first + n, c2 * half : (c2 + 1) * half, :] = placed.astype(BF).astype(F32)

    def one_mode(k, carry):
        total = None
        for c in range(channels):
            term = modal_ref[k, c : c + 1, :owned] * w_ref[k, c].astype(F32)
            total = term if total is None else total + term
        mixed_ref[k, :, :owned] = total
        return carry

    lax.fori_loop(0, modes_x, one_mode, 0)
    for k in range(modes_x):
        for i in range(per):
            placed = None
            for q in range(4):
                c2 = q // 2
                piece = mixed_ref[k, c2 * half : (c2 + 1) * half, :]
                shift = (KZ * q - KZ * i) % LANES
                piece = pltpu.roll(piece, shift, 1) if shift else piece
                placed = piece if placed is None else jnp.where(quarter == q, piece, placed)
            spread_ref[k, i * half : (i + 1) * half, :] = placed
    for a in range(members):
        total = None
        for k in range(modes_x):
            term = spread_ref[k] * tv_ref[k * members + a][None, :]
            total = term if total is None else total + term
        out_ref[a] = total


def fine_mixed(received, weights, local_x):
    members, rows, _ = received.shape
    _, modes_x, channels, _ = weights.shape
    table = cosine(modes_x, members * local_x).reshape(modes_x * members, local_x)
    lanes = np.tile(np.repeat(table, KZ, axis=1), (1, 2)).astype(np.float32)
    return vmem_call(
        mix_fine,
        [(received.shape, F32)],
        (received, jnp.transpose(weights, (1, 2, 3, 0)), jnp.asarray(lanes)),
        [
            pltpu.VMEM((modes_x, channels, LANES), F32),
            pltpu.VMEM((modes_x, channels, LANES), F32),
            pltpu.VMEM((modes_x, rows, LANES), F32),
        ],
        16,
    )


def lift_block(source, parts, y, store):
    channels = source.shape[0]
    block = jnp.concatenate(
        [source[:, y + s : y + s + 8, :].reshape(channels * 8, LANES) for s in (0, 8)], axis=1
    )
    high, low = split(block)
    done = dot(parts[0], high) + dot(parts[1], high) + dot(parts[0], low)
    for n in range(2):
        store(y + 8 * n, done[:, n * LANES : (n + 1) * LANES].reshape(channels, 8, LANES))


def stripes(source, target, sems, first, step):
    copies = []
    for n, y in enumerate(range(0, source.shape[-2], step)):
        span = (slice(None),) * (len(source.shape) - 2) + (pl.ds(y, step), slice(None))
        copies.append(pltpu.make_async_copy(source.at[span], target.at[span], sems.at[first + n]))
    return copies


def coarse_table(table_ref, out_ref):
    lane = lax.broadcasted_iota(jnp.int32, table_ref.shape[1:], 1) % GROUP
    cells_z = table_ref.shape[1]
    for c in range(GROUP):
        for part in range(2):
            out_ref[part, c * cells_z : (c + 1) * cells_z, :] = jnp.where(
                lane == c, table_ref[part].astype(F32), 0.0
            ).astype(BF)


def lift_fine_kernel(hbm_ref, a_ref, ec_ref, out_hbm, w_ref, v_ref, out_ref, sems):
    _, local_x, _, _ = v_ref.shape
    fetches = stripes(hbm_ref, v_ref, sems, 0, 32)
    stores = stripes(out_ref, out_hbm, sems, len(fetches), 32)
    for copy in fetches:
        copy.start()
    coarse_table(ec_ref, w_ref)
    parts = interleave_matrix(a_ref[...])
    for n in range(len(fetches)):
        fetches[n].wait()
        for x in range(local_x):
            def store(at, value, x=x):
                out_ref[:, x, at : at + 8, :] = value

            for y in range(32 * n, 32 * n + 32, 16):
                lift_block(v_ref.at[:, x], parts, y, store)
        stores[n].start()
    for copy in stores:
        copy.wait()


def project_kernel(hbm_ref, a_ref, base_hbm, out_hbm, v_ref, base_ref, sems):
    _, local_x, cells_y, _ = v_ref.shape
    steps = cells_y // 32
    fetches = stripes(hbm_ref, v_ref, sems, 0, 32)
    bases = stripes(base_hbm, base_ref, sems, steps, 32)
    stores = stripes(base_ref, out_hbm, sems, 2 * steps, 32)
    for n in range(steps):
        fetches[n].start()
        bases[n].start()
    parts = interleave_matrix(a_ref[...])
    for n in range(steps):
        fetches[n].wait()
        bases[n].wait()
        for x in range(local_x):
            def store(at, value, x=x):
                base_ref[:, x, at : at + 8, :] += value

            for y in range(32 * n, 32 * n + 32, 16):
                lift_block(v_ref.at[:, x], parts, y, store)
        stores[n].start()
    for copy in stores:
        copy.wait()


def fine_lifted(features, matrix):
    _, _, cells_y, cells_z = features.shape
    coarse_z = cells_z // 2
    pool_z = np.kron(np.eye(coarse_z), np.ones((1, 2))) / 2.0
    ec = np.repeat((cosine(KZ // 2, coarse_z) @ pool_z).T, GROUP, axis=1)
    ec = np.stack(halves(ec))
    return vmem_call(
        lift_fine_kernel,
        [(features.shape, F32), ((2, GROUP * cells_z, 2 * LANES), BF)],
        (features, matrix, jnp.asarray(ec)),
        [
            pltpu.VMEM(features.shape, F32),
            pltpu.VMEM(features.shape, F32),
            pltpu.SemaphoreType.DMA((cells_y // 16,)),
        ],
        20,
        LIFT_FLOPS,
        in_hbm=(0,),
        out_hbm=(0,),
    )


def projected(level_one, matrix, features):
    cells_y = features.shape[2]
    return vmem_call(
        project_kernel,
        [(features.shape, F32)],
        (level_one, matrix, features),
        [
            pltpu.VMEM(features.shape, F32),
            pltpu.VMEM(features.shape, F32),
            pltpu.SemaphoreType.DMA((3 * cells_y // 32,)),
        ],
        20,
        LIFT_FLOPS,
        in_hbm=(0, 2),
        out_hbm=(0,),
    )


def lift_coarse_kernel(hbm_ref, a_ref, pz_ref, o_ref, ei_ref, out_ref, parts_ref, b_ref, p_ref, v_ref, sem):
    fetch = pltpu.make_async_copy(hbm_ref, v_ref, sem)
    fetch.start()
    parts = interleave_matrix(o_ref[...])
    parts_ref[0] = parts[0]
    parts_ref[1] = parts[1]
    parts = interleave_matrix(a_ref[...])
    fetch.wait()
    channels, cells_y, _ = v_ref.shape

    def store(y, value):
        p_ref[:, y : y + 8, :] = value

    for y in range(0, cells_y, 16):
        lift_block(v_ref, parts, y, store)
    rows = jnp.concatenate(
        [jnp.concatenate([p_ref[c], p_ref[c + 1]], axis=1) for c in range(0, channels, 2)], axis=0
    )
    high, low = split(rows)
    done = dot(high, pz_ref[...]) + dot(low, pz_ref[...])
    for cg in range(channels // GROUP):
        for t in range(GROUP // 2):
            n = cg * (GROUP // 2) + t
            out_ref[cg * cells_y : (cg + 1) * cells_y, t * LANES : (t + 1) * LANES] = done[
                n * cells_y : (n + 1) * cells_y
            ]
    coarse_z = pz_ref.shape[1] // 2
    lane = lax.broadcasted_iota(jnp.int32, (2 * LANES, LANES), 1) // coarse_z
    row = lax.broadcasted_iota(jnp.int32, (2 * LANES, LANES), 0) % GROUP
    for t in range(GROUP // 2):
        for part in range(2):
            b_ref[part, :, t * LANES : (t + 1) * LANES] = jnp.where(
                row == 2 * t + lane, ei_ref[part].astype(F32), 0.0
            ).astype(BF)


def coarse_lifted(pool_y, lift_middle, project_out):
    channels, coarse_y, cells_z = pool_y.shape
    coarse_z = cells_z // 2
    pool_z = np.kron(np.eye(coarse_z), np.ones((1, 2))).T / 2.0
    pool_z = np.kron(np.eye(2), pool_z).astype(BF)
    inverse_z = np.repeat(cosine(KZ // 2, coarse_z), GROUP, axis=0)
    ei = np.stack(halves(np.concatenate([inverse_z] * (LANES // coarse_z), axis=1)))
    wide = GROUP // 2 * LANES
    return vmem_call(
        lift_coarse_kernel,
        [
            ((channels // GROUP * coarse_y, wide), F32),
            ((2, channels * 8, channels * 8), BF),
            ((2, 2 * LANES, wide), BF),
        ],
        (pool_y, lift_middle, jnp.asarray(pool_z), project_out, jnp.asarray(ei)),
        [
            pltpu.VMEM(pool_y.shape, F32),
            pltpu.VMEM(pool_y.shape, F32),
            pltpu.SemaphoreType.DMA,
        ],
        12,
        LIFT_FLOPS // 2,
        in_hbm=(0,),
    )


def inverse_fine(r_ref, lift_hbm, ty_ref, bz_ref, yc_ref, w_ref, level_hbm, pool_hbm, out_ref,
                 g_ref, q_ref, d_ref, lift_ref, level_ref, tall_ref, pool_ref, sems, place):
    _, half, local_x, cells_y, _ = lift_ref.shape
    modes_y = r_ref.shape[0] // half
    half_ky = modes_y // 2
    steps = FETCHES
    chunk = half // steps
    spans = [pl.ds(n * chunk, chunk) for n in range(steps)]
    fetches = [
        pltpu.make_async_copy(lift_hbm.at[:, span], lift_ref.at[:, span], sems.at[n])
        for n, span in enumerate(spans)
    ]
    stores = [
        pltpu.make_async_copy(level_ref.at[:, span], level_hbm.at[:, span], sems.at[steps + n])
        for n, span in enumerate(spans)
    ]
    pool = pltpu.make_async_copy(pool_ref, pool_hbm, sems.at[2 * steps])
    for copy in fetches:
        copy.start()
    for cp in range(0, half, 2):
        block = jnp.concatenate(
            [r_ref[pl.ds(cp + n, modes_y, stride=half), :] for n in range(2)], axis=1
        )
        high, low = split(block)
        both = dot(ty_ref[...], jnp.concatenate([high, low, high], axis=0)).astype(BF)
        for n in range(2):
            part = both[:, n * LANES : (n + 1) * LANES]
            g_ref[(cp + n) * cells_y : (cp + n + 1) * cells_y, :] = jnp.concatenate(
                [part, part], axis=1
            )
    for step in range(steps):
        first = step * chunk
        fetches[step].wait()
        wide = dot(g_ref[first * cells_y : (first + chunk) * cells_y, :], bz_ref[...])
        for n in range(chunk):
            cp = first + n
            for c2 in range(2):
                for x in range(local_x):
                    q = c2 * local_x + x
                    piece = wide[n * cells_y : (n + 1) * cells_y, q * LANES : (q + 1) * LANES]
                    piece = gelu(piece + lift_ref[c2, cp, x])
                    level_ref[c2, cp, x] = piece
                    tall_ref[cp, x * cells_y : (x + 1) * cells_y, c2 * LANES : (c2 + 1) * LANES] = (
                        piece.astype(BF)
                    )
        stores[step].start()
    for cp in range(half):
        down = dot(yc_ref[...], tall_ref[cp])
        for c2 in range(2):
            c = cp + c2 * half
            cg, inner = c // GROUP, c % GROUP
            part = down[:, c2 * LANES : (c2 + 1) * LANES]
            q_ref[cg * half_ky : (cg + 1) * half_ky, inner * LANES : (inner + 1) * LANES] = (
                part[:half_ky] + part[half_ky : 2 * half_ky]
            )
            pool_ref[c] = part[2 * half_ky :]
    pool.start()
    high, low = split(q_ref[...])
    d_ref[...] = dot(high, w_ref[0]) + dot(low, w_ref[0]) + dot(high, w_ref[1])
    out_ref[...] = jnp.zeros_like(out_ref)
    for (cg, jh, i), row in place.items():
        source = cg * half_ky + i
        out_ref[row : row + 1, :] = d_ref[source : source + 1, jh * LANES : (jh + 1) * LANES]
    for copy in stores:
        copy.wait()
    pool.wait()


def fine_level(received, lifted, table_z, place, place_rows):
    channels, local_x, cells_y, cells_z = lifted.shape
    half_ky = KY // 2
    coarse_y = cells_y // 2
    high, low = halves(cosine(KY, cells_y).T)
    ty = np.concatenate([high, high, low], axis=1)
    eye = np.eye(2 * local_x, dtype=np.float32)
    bz = np.concatenate(
        [np.kron(eye, part.astype(np.float32)) for part in halves(cosine(KZ, cells_z))], axis=0
    ).astype(BF)
    pool_y = np.kron(np.eye(coarse_y), np.ones((1, 2))) / (2.0 * local_x)
    high, low = halves(cosine(half_ky, coarse_y) @ pool_y)
    yc = np.concatenate([high, low, pool_y.astype(BF)], axis=0)
    yc = np.concatenate([yc] * local_x, axis=1)
    groups = channels // GROUP

    def inverse_fine_kernel(*refs):
        inverse_fine(*refs, place)

    whole = paired(lifted).shape
    level, pooled, coarse = vmem_call(
        inverse_fine_kernel,
        [(whole, F32), ((channels, coarse_y, cells_z), F32), ((place_rows, LANES), F32)],
        (received, paired(lifted), jnp.asarray(ty), jnp.asarray(bz), jnp.asarray(yc), table_z),
        [
            pltpu.VMEM((channels // 2 * cells_y, 2 * LANES), BF),
            pltpu.VMEM((groups * half_ky, GROUP * cells_z), F32),
            pltpu.VMEM((groups * half_ky, 2 * LANES), F32),
            pltpu.VMEM(whole, F32),
            pltpu.VMEM(whole, F32),
            pltpu.VMEM((channels // 2, local_x * cells_y, 2 * LANES), BF),
            pltpu.VMEM((channels, coarse_y, cells_z), F32),
            pltpu.SemaphoreType.DMA((2 * FETCHES + 1,)),
        ],
        24,
        in_hbm=(1,),
        out_hbm=(0, 1),
    )
    return level.reshape(lifted.shape), pooled, coarse


def mix_coarse(r_ref, w_ref, out_ref, table, rows):
    members, pad, _ = r_ref.shape
    owned, modes_x, channels, _ = w_ref.shape
    groups = channels // GROUP
    inner = LANES // GROUP
    units = owned // inner
    lane = lax.broadcasted_iota(jnp.int32, (rows, LANES), 1)
    row = lax.broadcasted_iota(jnp.int32, (rows, channels), 0)
    modal = []
    for k in range(modes_x):
        total = None
        for a in range(members):
            term = r_ref[a] * float(table[k, a])
            total = term if total is None else total + term
        modal.append(total)
    fill = jnp.zeros((rows - modes_x * units, LANES), F32)
    packed = [
        jnp.concatenate(
            [modal[k][cg * units : (cg + 1) * units] for k in range(modes_x)] + [fill], axis=0
        )
        for cg in range(groups)
    ]
    mixed = []
    for j in range(inner):
        placed = None
        for cg in range(groups):
            shift = (GROUP * cg - GROUP * j) % LANES
            piece = pltpu.roll(packed[cg], shift, 1) if shift else packed[cg]
            placed = piece if placed is None else jnp.where(lane // GROUP == cg, piece, placed)
        left = placed[:, :channels].astype(BF)
        total = jnp.zeros((rows, channels), F32)
        for k in range(modes_x):
            for u in range(units):
                full = dot(left, w_ref[u * inner + j, k])
                total = jnp.where(row == k * units + u, full, total)
        mixed.append(jnp.concatenate([total, jnp.zeros((rows, LANES - channels), F32)], axis=1))
    spread = []
    for cg in range(groups):
        placed = None
        for j in range(inner):
            shift = (GROUP * j - GROUP * cg) % LANES
            piece = pltpu.roll(mixed[j], shift, 1) if shift else mixed[j]
            placed = piece if placed is None else jnp.where(lane // GROUP == j, piece, placed)
        spread.append(placed)
    final = []
    for k in range(modes_x):
        final.append(
            jnp.concatenate(
                [spread[cg][k * units : (k + 1) * units] for cg in range(groups)]
                + [jnp.zeros((pad - groups * units, LANES), F32)],
                axis=0,
            )
        )
    for a in range(members):
        total = None
        for k in range(modes_x):
            term = final[k] * float(table[k, a])
            total = term if total is None else total + term
        out_ref[a] = total


def coarse_mixed(received, weights, coarse_x):
    owned, modes_x, _, _ = weights.shape
    table = cosine(modes_x, coarse_x)
    units = owned * GROUP // LANES
    rows = -(-modes_x * units // 16) * 16

    def mix_coarse_kernel(*refs):
        mix_coarse(*refs, table, rows)

    return vmem_call(mix_coarse_kernel, [(received.shape, F32)], (received, weights), [], 8)


def finish(r_ref, lift_ref, base_hbm, parts_ref, b_ref, yi_ref, up_ref, out_hbm, l_ref, u_ref, res_ref, sems):
    channels, local_x, cells_y, _ = res_ref.shape
    coarse_y = cells_y // 2
    groups = channels // GROUP
    fetches = stripes(base_hbm, res_ref, sems, 0, 32)
    stores = stripes(res_ref, out_hbm, sems, len(fetches), 32)
    for copy in fetches:
        copy.start()
    high, low = split(r_ref[...])
    grid = dot(yi_ref[0], high) + dot(yi_ref[0], low) + dot(yi_ref[1], high)
    left = jnp.concatenate(
        [
            jnp.concatenate(
                [grid[(2 * cg + jh) * coarse_y : (2 * cg + jh + 1) * coarse_y] for jh in range(2)],
                axis=1,
            )
            for cg in range(groups)
        ],
        axis=0,
    )
    high, low = split(left)
    level = dot(high, b_ref[0]) + dot(low, b_ref[0]) + dot(high, b_ref[1])
    level = gelu(level + lift_ref[...])
    for cg in range(groups):
        tall = jnp.concatenate(
            [
                level[cg * coarse_y : (cg + 1) * coarse_y, t * LANES : (t + 1) * LANES]
                for t in range(GROUP // 2)
            ],
            axis=0,
        )
        high, low = split(tall)
        wide = dot(jnp.concatenate([high, low], axis=1), up_ref[...])
        for t in range(GROUP // 2):
            for c2 in range(2):
                l_ref[cg * GROUP + 2 * t + c2] = wide[
                    t * coarse_y : (t + 1) * coarse_y, c2 * LANES : (c2 + 1) * LANES
                ]

    def store(y, value):
        for c in range(channels):
            for n in range(2):
                u_ref[pl.ds(c * cells_y + 2 * y + n, 8, stride=2), :] = value[c]

    parts = (parts_ref[0], parts_ref[1])
    lift_block(l_ref, parts, 0, store)
    for n, y in enumerate(range(0, coarse_y, 16)):
        fetches[n].wait()
        if y + 16 < coarse_y:
            lift_block(l_ref, parts, y + 16, store)
        for c in range(channels):
            piece = u_ref[c * cells_y + 2 * y : c * cells_y + 2 * y + 32, :]
            for x in range(local_x):
                res_ref[c, x, 2 * y : 2 * y + 32, :] += piece
        stores[n].start()
    for copy in stores:
        copy.wait()


def final_result(received, lifted, base, parts, inverse_z, place, place_rows):
    channels, _, cells_y, cells_z = base.shape
    half_ky = KY // 2
    coarse_y, coarse_z = cells_y // 2, cells_z // 2
    groups = channels // GROUP
    table_y = cosine(half_ky, coarse_y)
    left = np.zeros((groups, 2, coarse_y, place_rows))
    for (cg, jh, i), row in place.items():
        left[cg, jh, :, row] = table_y[i]
    yi = np.stack(halves(left.reshape(groups * 2 * coarse_y, place_rows)))
    up = np.kron(np.eye(2), np.kron(np.eye(coarse_z), np.ones((1, 2))))
    up = np.concatenate([up, up], axis=0).astype(BF)
    return vmem_call(
        finish,
        [(base.shape, F32)],
        (received, lifted, base, parts, inverse_z, jnp.asarray(yi), jnp.asarray(up)),
        [
            pltpu.VMEM((channels, coarse_y, cells_z), F32),
            pltpu.VMEM((channels * cells_y, LANES), F32),
            pltpu.VMEM(base.shape, F32),
            pltpu.SemaphoreType.DMA((2 * cells_y // 32,)),
        ],
        24,
        in_hbm=(2,),
        out_hbm=(0,),
    )


def swap(blocks):
    return lax.all_to_all(blocks, "gx", split_axis=0, concat_axis=0, tiled=True)


def plain_mix(coeffs, weights, cells_x):
    table_x = jnp.asarray(cosine(weights.shape[1], cells_x), F32)
    pencils = lax.all_to_all(coeffs, "gx", split_axis=0, concat_axis=1, tiled=True)
    modal = jnp.einsum("mxc,kx->mkc", pencils, table_x, precision=HIGHEST)
    mixed = jnp.einsum(
        "mkc,mkco->mko", modal.astype(BF), weights, preferred_element_type=F32
    )
    back = jnp.einsum("mkc,kx->mxc", mixed, table_x, precision=HIGHEST)
    return lax.all_to_all(back, "gx", split_axis=1, concat_axis=0, tiled=True)


def on_device(features, fine_weights, middle_weights, lift_fine, lift_middle, project_out):
    channels, local_x, _, _ = features.shape
    group_size = lax.axis_size("gx")
    cells_x = local_x * group_size
    half = channels // 2
    half_ky, half_kz = KY // 2, KZ // 2
    groups = channels // GROUP
    inner = LANES // GROUP

    coeffs = fine_coefficients(features)
    owned = fine_weights.shape[0]
    if owned % KZ == 0 and owned <= LANES:
        received = swap(coeffs.reshape(group_size, -1, LANES))
        mixed = fine_mixed(received, fine_weights, local_x)
        slabs = swap(mixed).reshape(coeffs.shape)
    else:
        modes = coeffs.reshape(KY, half, 2, local_x, KZ).transpose(0, 4, 3, 2, 1)
        slabs = plain_mix(modes.reshape(KY * KZ, local_x, channels), fine_weights, cells_x)
        slabs = slabs.reshape(KY, KZ, local_x, 2, half).transpose(0, 4, 3, 2, 1)
        slabs = slabs.reshape(coeffs.shape)
    lifted, table_z = fine_lifted(features, lift_fine)

    owned = middle_weights.shape[0]
    direct = owned % inner == 0 and groups * (owned // inner) <= PAD
    place = {}
    for cg in range(groups):
        for i in range(half_ky):
            for jh in range(2):
                if direct:
                    member, unit = divmod(2 * i + jh, owned // inner)
                    place[cg, jh, i] = member * PAD + cg * (owned // inner) + unit
                else:
                    place[cg, jh, i] = (jh * groups + cg) * half_ky + i
    place_rows = group_size * PAD if direct else 2 * groups * half_ky
    level_one, pool_y, coarse = fine_level(slabs, lifted, table_z, place, place_rows)
    base = projected(level_one, project_out, features)
    coarse_lift, parts, inverse_z = coarse_lifted(pool_y, lift_middle, project_out)
    coarse_x = cells_x // 2
    if direct:
        received = swap(coarse.reshape(group_size, PAD, LANES))
        mixed = coarse_mixed(received, middle_weights, coarse_x)
        slabs = swap(mixed).reshape(coarse.shape)
    else:
        modes = coarse.reshape(2, groups, half_ky, inner, GROUP).transpose(2, 0, 3, 1, 4)
        slabs = plain_mix(
            modes.reshape(half_ky * half_kz, 1, channels), middle_weights, coarse_x
        )
        slabs = slabs.reshape(half_ky, 2, inner, groups, GROUP).transpose(1, 3, 0, 2, 4)
        slabs = slabs.reshape(coarse.shape)
    return final_result(slabs, coarse_lift, base, parts, inverse_z, place, place_rows)


def solution(mesh):
    in_specs = (
        P(None, ("groups", "gx"), None, None),
        P("gx", None, None, None),
        P("gx", None, None, None),
        P(),
        P(),
        P(),
    )
    out_specs = P(None, ("groups", "gx"), None, None)

    return jax.shard_map(
        on_device, mesh=mesh, in_specs=in_specs, out_specs=out_specs, check_vma=False
    )
```
